256 devices in a mesh: row: 8 (over y, core), col: 32 (over x, z).
Axes of the slice: x: 4, y: 4, z: 8, core: 2. Of those that a mesh axis runs over, the one named last changes fastest.
Arguments:
- adjacency: int32 [16384, 32768], P('row', 'col'), may hold values from 0 to 1, as said below
Outputs:
- closure: bfloat16 [16384, 32768], P('row', 'col')
The draws below stay inside these ranges and needn't reach their ends.
Inputs may be any that keep to these rules, and one draw needn't show every extreme that they name: `adjacency`: every entry is 0 or 1; there is no bound on the number of ones in a row, a column or a block, and their share differs widely between rows and between columns.
All inputs are finite; a program needn't handle non-finite values.
Results may differ from the reference program's by a relative error of at most 0.001.
Values may be sent and summed in bfloat16 or wider, within the bound.
A program may use at most 192 MiB of HBM per device.

```python
import math
import jax
import jax.numpy as jnp
from jax import lax

PANEL = 512
PANELS = 4
ROWS = 16384
VERTS = 32768


def draw_adjacency(key, part):
    window = PANELS * PANEL
    scale_top = 1 << 20
    plain_level = scale_top // math.isqrt(window)
    sparse_level = scale_top // window
    dense_level = scale_top // 2
    key_hubs, key_levels, key_dense, key_entries = jax.random.split(jax.random.fold_in(key, 7), 4)
    hub_flags = (jax.random.randint(key_hubs, (window,), 0, 3, dtype=jnp.int32) < 2).astype(jnp.int32)
    column_hub = jnp.concatenate([hub_flags, jnp.zeros((VERTS - window,), jnp.int32)])
    row_hub = jnp.concatenate([hub_flags, jnp.zeros((ROWS - window,), jnp.int32)])
    row_ids = jnp.arange(ROWS, dtype=jnp.int32)
    levels = jax.random.randint(key_levels, (ROWS,), 0, 3, dtype=jnp.int32)
    row_plain = jnp.where(levels == 0, plain_level // 2, jnp.where(levels == 1, plain_level, plain_level * 2))
    dense_pick = jax.random.randint(key_dense, (ROWS,), 0, 16, dtype=jnp.int32)
    dense_row = (dense_pick == 0) & (row_ids >= window) | (row_hub == 1)
    on_plain = jnp.where(dense_row, dense_level, row_plain).astype(jnp.int32)
    threshold = jnp.where(column_hub[None, :] == 1, jnp.int32(sparse_level), on_plain[:, None])
    entry_draws = jax.random.randint(key_entries, (ROWS, VERTS), 0, scale_top, dtype=jnp.int32)
    return (entry_draws < threshold).astype(jnp.int32)


def setup_inputs(seed: int = 0) -> dict:
    streams_of = jax.random.split(jax.random.key(seed), 2)
    return {
        "adjacency": draw_adjacency(jax.random.fold_in(streams_of[1], 71), 0),
    }


def reference(adjacency):
    window_cols = PANELS * PANEL
    right_rows = adjacency[:window_cols].astype(jnp.float32)
    block = math.gcd(ROWS, 2048)
    blocks = adjacency.reshape(ROWS // block, block, VERTS)

    def close_rows(rows_int):
        counts = jnp.dot(rows_int[:, :window_cols].astype(jnp.float32), right_rows,
                         precision=lax.Precision.HIGHEST, preferred_element_type=jnp.float32)
        return jnp.where(counts > 0.5, 1.0, rows_int.astype(jnp.float32)).astype(jnp.bfloat16)

    return lax.map(close_rows, blocks).reshape(ROWS, VERTS)
```

```python
import jax
import jax.numpy as jnp
from jax import lax
from jax.experimental import pallas as pl
from jax.experimental.pallas import tpu as pltpu
from jax.sharding import PartitionSpec as P

MESH = pl.DeviceIdType.MESH
XS, ZS, YS = 4, 8, 4
ROOTS = 2
STEPS = ((0, 1), (0, -1), (1, 0), (-1, 0))
TREES = (
    ".0000000122232031212001113313002",
    ".1111111031120220001130302132333",
    ".3333333200011112120222221221220",
    ".2222222313303303333313030000111",
)
CHUNK = 16
LAG = 2.2
RCHUNK = 64
RLAG = 2
PIECE = 128
BLOCK = 256
FIRST = 26
EVERY = 3


def tables():
    depths, children = [], []
    for tree in TREES:
        parent = {}
        for p, c in enumerate(tree):
            if c != ".":
                dx, dz = STEPS[int(c)]
                parent[p] = ((p // ZS - dx) % XS * ZS + (p % ZS - dz) % ZS, int(c))
        depth = []
        for p in range(XS * ZS):
            d, q = 0, p
            while q in parent:
                d, q = d + 1, parent[q][0]
            depth.append(d)
        depths.append(depth)
        kids = [[0] * (XS * ZS) for _ in range(4)]
        for u, c in parent.values():
            kids[c][u] = 1
        children.append(kids)
    return depths, children


DEPTHS, CHILDREN = tables()
LAGS = [[round(LAG * d) for d in depth] for depth in DEPTHS]
MAX_LAG = max(map(max, LAGS))


def lookup(values, p):
    total = jnp.int32(0)
    for bit in range(max(values).bit_length()):
        mask = sum(((v >> bit) & 1) << i for i, v in enumerate(values))
        mask = mask - (1 << 32) if mask >= 1 << 31 else mask
        total = total + (lax.shift_right_logical(jnp.int32(mask), p) & 1) * (1 << bit)
    return total


def kernel(adj_ref, out_ref, stage, own, left, right, load_sem, recv_sem, send_sem, ring_sem, ring_send, pair_sem, pair_send):
    rows, cols = own.shape
    chunks = rows // (4 * CHUNK)
    half = rows // 2
    rchunks = half // RCHUNK
    pieces = rows // PIECE
    row, col = lax.axis_index("row"), lax.axis_index("col")
    y, core = row // 2, row % 2
    x, z = col // ZS, col % ZS
    towards = [lax.rem(x + dx + XS, XS) * ZS + lax.rem(z + dz + ZS, ZS) for dx, dz in STEPS]
    partner = row + 1 - 2 * core
    up, down = lax.rem(y + 1, YS) * 2 + core, lax.rem(y + YS - 1, YS) * 2 + core

    barrier = pltpu.get_barrier_semaphore()
    for c in towards:
        pl.semaphore_signal(barrier, inc=1, device_id=(row, c), device_id_type=MESH)
    for r in (partner, up, down):
        pl.semaphore_signal(barrier, inc=1, device_id=(r, col), device_id_type=MESH)

    def load(i):
        part = pl.ds(i * PIECE, PIECE)
        return pltpu.make_async_copy(adj_ref.at[part, :], stage.at[part, :], load_sem.at[i])

    def convert(i):
        load(i).wait()
        part = pl.ds(pl.multiple_of(i * PIECE, PIECE), PIECE)
        piece = stage[part, :].astype(jnp.float32).astype(jnp.bfloat16)
        own[part, :] = piece
        for s in range(ROOTS):
            @pl.when(col == s)
            def _():
                left[s, part, :] = piece

        @pl.when(row == 0)
        def _():
            right[part, :] = piece

    for i in range(pieces):
        load(i).start()
    convert(0)

    trees = []
    for s in range(ROOTS):
        p = x * ZS + lax.rem(z - s + ZS, ZS)
        for t in range(4):
            lag = lookup(LAGS[t], p)
            kids = [lookup(CHILDREN[t][d], p) for d in range(4)]
            trees.append((s, t, lag, kids))

    def tree_copy(s, t, k, d):
        part = pl.ds(pl.multiple_of((k * 4 + t) * CHUNK, CHUNK), CHUNK)
        ref = left.at[s, part, :]
        return pltpu.make_async_remote_copy(
            src_ref=ref, dst_ref=ref, send_sem=send_sem.at[s * 4 + t, d], recv_sem=recv_sem.at[s * 4 + t, k],
            device_id=(row, towards[d]), device_id_type=MESH,
        )

    hop = jnp.where(core == 0, y, lax.rem(YS - y, YS))
    onward = jnp.where(core == 0, up, down)

    def ring_part(k, h):
        return right.at[pl.ds(pl.multiple_of((2 * k + h) * RCHUNK, RCHUNK), RCHUNK), :]

    def ring_copy(k, h, device):
        ref = ring_part(k, h)
        return pltpu.make_async_remote_copy(
            src_ref=ref, dst_ref=ref, send_sem=ring_send, recv_sem=ring_sem.at[k], device_id=(device, col), device_id_type=MESH,
        )

    def pair_copy(k, h):
        ref = ring_part(k, h)
        return pltpu.make_async_remote_copy(
            src_ref=ref, dst_ref=ref, send_sem=pair_send, recv_sem=pair_sem, device_id=(partner, col), device_id_type=MESH,
        )

    pl.semaphore_wait(barrier, 7)

    def multiply(b):
        part = pl.ds(pl.multiple_of(b * BLOCK, BLOCK), BLOCK)
        width = 256

        @pl.loop(0, cols // width)
        def _(j):
            span = pl.ds(pl.multiple_of(j * width, width), width)
            counts = jnp.dot(left[0, part, :], right[:half, span], preferred_element_type=jnp.float32)
            counts = counts + jnp.dot(left[1, part, :], right[half:, span], preferred_element_type=jnp.float32)
            out_ref[part, span] = jnp.where(counts > 0.5, 1.0, own[part, span].astype(jnp.float32)).astype(jnp.bfloat16)

    steps = FIRST + EVERY * (rows // BLOCK - 1) + 1

    def step(n, carry):
        k = n - hop * RLAG - core

        @pl.when((k >= 0) & (k < rchunks))
        def _():
            @pl.when(row != 0)
            def _():
                ring_copy(k, core, onward).wait_recv()

            @pl.when(hop < YS - 1)
            def _():
                ring_copy(k, core, onward).start()

            @pl.when(row != 1)
            def _():
                pair_copy(k, core).start()

            @pl.when(row == 0)
            def _():
                ring_copy(k, 1, partner).start()

        for s, t, lag, kids in trees:
            k = n - lag

            @pl.when((k >= 0) & (k < chunks))
            def _(s=s, t=t, k=k, kids=kids):
                @pl.when(col != s)
                def _():
                    tree_copy(s, t, k, 0).wait_recv()

                for d in range(4):
                    if max(CHILDREN[t][d]):
                        @pl.when(kids[d] == 1)
                        def _(d=d):
                            tree_copy(s, t, k, d).start()

        @pl.when(n + 1 < pieces)
        def _():
            convert(n + 1)

        @pl.when(n == FIRST - 1)
        def _():
            @pl.when(row != 0)
            def _():
                ref = right.at[pl.ds(0, half), :]
                pltpu.make_async_remote_copy(
                    src_ref=ref, dst_ref=ref, send_sem=pair_send, recv_sem=pair_sem, device_id=(partner, col),
                    device_id_type=MESH,
                ).wait_recv()

        @pl.when((n >= FIRST) & (lax.rem(n - FIRST + EVERY, EVERY) == 0))
        def _():
            multiply((n - FIRST) // EVERY)

        return carry

    lax.fori_loop(0, steps, step, 0)

    for s, t, lag, kids in trees:
        for d in range(4):
            if max(CHILDREN[t][d]):
                @pl.when(kids[d] == 1)
                def _(s=s, t=t, d=d):
                    ref = left.at[0, pl.ds(0, chunks * CHUNK), :]
                    pltpu.make_async_remote_copy(
                        src_ref=ref, dst_ref=ref, send_sem=send_sem.at[s * 4 + t, d], recv_sem=recv_sem.at[0, 0],
                        device_id=(row, towards[d]), device_id_type=MESH,
                    ).wait_send()

    def drain(sem, other):
        ref = right.at[pl.ds(0, half), :]
        pltpu.make_async_remote_copy(
            src_ref=ref, dst_ref=ref, send_sem=sem, recv_sem=ring_sem.at[0], device_id=(other, col), device_id_type=MESH,
        ).wait_send()

    @pl.when(hop < YS - 1)
    def _():
        drain(ring_send, onward)

    @pl.when(row == 0)
    def _():
        drain(ring_send, partner)

    @pl.when(row != 1)
    def _():
        drain(pair_send, partner)


def per_device(adjacency):
    rows, cols = adjacency.shape
    chunks = rows // (4 * CHUNK)
    return pl.pallas_call(
        kernel,
        name="closure",
        out_shape=jax.ShapeDtypeStruct((rows, cols), jnp.bfloat16),
        in_specs=[pl.BlockSpec(memory_space=pl.ANY)],
        out_specs=pl.BlockSpec(memory_space=pltpu.VMEM),
        scratch_shapes=[
            pltpu.VMEM((rows, cols), jnp.int32),
            pltpu.VMEM((rows, cols), jnp.bfloat16),
            pltpu.VMEM((ROOTS, rows, cols), jnp.bfloat16),
            pltpu.VMEM((ROOTS * cols, cols), jnp.bfloat16),
            pltpu.SemaphoreType.DMA((rows // PIECE,)),
            pltpu.SemaphoreType.DMA((ROOTS * 4, chunks)),
            pltpu.SemaphoreType.DMA((ROOTS * 4, 4)),
            pltpu.SemaphoreType.DMA((rows // 2 // RCHUNK,)),
            pltpu.SemaphoreType.DMA,
            pltpu.SemaphoreType.DMA,
            pltpu.SemaphoreType.DMA,
        ],
        compiler_params=pltpu.CompilerParams(
            collective_id=0, has_side_effects=True, vmem_limit_bytes=48 * 1024 * 1024
        ),
    )(adjacency)


def solution(mesh):
    spec = P("row", "col")
    return jax.shard_map(per_device, mesh=mesh, in_specs=(spec,), out_specs=spec, check_vma=False)
```
